512 devices in a mesh: vir: 64 (over z, x_lo, core), occ: 8 (over y, x_hi).
Axes of the slice: x: 4 (x_hi: 2, x_lo: 2; x = x_hi * 2 + x_lo), y: 4, z: 16, core: 2. Of those that a mesh axis runs over, the one named last changes fastest.
Arguments:
- tau_amps: bfloat16 [4096, 32768], P('occ', 'vir'), may hold values from -6 to 6
- lambda_amps: bfloat16 [4096, 32768], P('occ', 'vir'), may hold values from -0.09375 to 0.09375
Outputs:
- density: float32 [32768, 5, 512], P(('vir', 'occ'))
The draws below stay inside these ranges and needn't reach their ends.
All inputs are finite; a program needn't handle non-finite values.
Results may differ from the reference program's by a relative error of at most 0.01.
Values may be sent and summed in bfloat16 or wider, within the bound.
A program may use at most 64 MiB of HBM per device.

```python
import jax
import jax.numpy as jnp
from jax import lax

O = 4096
P_DEV = 512
REACH = 4
P_SIZE = 32768
N_VIR = 64
N_OCC = 8


def steps_of(own_key, shape, shards, smallest, largest):
    gain, own = 1.0, jax.random.fold_in(own_key, 6)
    for position, shards_of in shards:
        draws = jnp.exp(jax.random.uniform(jax.random.fold_in(own, position), (shards_of,), jnp.float32, smallest / len(shards), largest / len(shards)))
        gain = gain * jnp.repeat(draws, shape[position] // shards_of).reshape([-1 if axis == position else 1 for axis in range(len(shape))])
    return gain


def normal_values(rng, dims, deviation, most, cuts=(), held_as=jnp.bfloat16):
    level = steps_of(rng, dims, cuts, -0.22, 0.18) if cuts else 1.0
    array = jax.random.normal(rng, dims, jnp.float32) * deviation * level
    return jnp.minimum(jnp.maximum(array, -most), most).astype(held_as)


def setup_inputs(seed: int = 0) -> dict:
    keys = jax.random.split(jax.random.key(seed), 3)
    return {
        "tau_amps": normal_values(keys[0], (O, P_SIZE), 1.0, 6.0, ((0, 8), (1, 64))),
        "lambda_amps": normal_values(keys[1], (O, P_SIZE), O ** -0.5, 0.09375, ((0, 8), (1, 64))),
    }


def reference(tau_amps, lambda_amps):
    tau_split = tau_amps.astype(jnp.float32).reshape(N_OCC, O // N_OCC, N_VIR, P_DEV)
    lambda_split = lambda_amps.astype(jnp.float32).reshape(N_OCC, O // N_OCC, N_VIR, P_DEV)

    def one_block(row_block):
        tau_rows = lax.dynamic_index_in_dim(tau_split, row_block, 2, keepdims=False)
        lambda_rows = lax.dynamic_index_in_dim(lambda_split, row_block, 2, keepdims=False)
        results = []
        for offset in range(REACH + 1):
            column = ((row_block + offset) % N_VIR).astype(jnp.int32)
            tau_cols = lax.dynamic_index_in_dim(tau_split, column, 2, keepdims=False)
            lambda_cols = lax.dynamic_index_in_dim(lambda_split, column, 2, keepdims=False)
            partial_terms = 0.5 * (jnp.einsum("gip,giq->gpq", tau_rows, lambda_cols)
                                   + jnp.einsum("gip,giq->gpq", lambda_rows, tau_cols))
            rounded = lax.optimization_barrier(partial_terms.astype(jnp.bfloat16))
            results.append(jnp.sum(rounded.astype(jnp.float32), axis=0))
        return jnp.stack(results, 0)

    blocks = lax.map(one_block, jnp.arange(N_VIR, dtype=jnp.int32))
    return blocks.transpose(0, 2, 1, 3).reshape(N_VIR * P_DEV, REACH + 1, P_DEV)
```

```python
import jax
import jax.numpy as jnp
from jax import lax
from jax.experimental import pallas as pl
from jax.experimental.pallas import tpu as pltpu
from jax.sharding import PartitionSpec as P

MESH = pl.DeviceIdType.MESH
REACH = 4
LANES = 128
F32 = jnp.float32


def kernel(tau_ref, lam_ref, out_ref, blk, lt, part, r1, s1, r2, xs, xr, fin,
           in_sem, zs, zr, xss, xrs, d1s, d1r, d2s, d2r, as_, ar, bs, br, hs, hr):
    depth = tau_ref.shape[0]
    pieces = tau_ref.shape[1] // LANES
    units = 2 * pieces
    rows = out_ref.shape[1]
    n_vir, n_occ = lax.axis_size("vir"), lax.axis_size("occ")
    n_y = n_occ // 2
    v, o = lax.axis_index("vir"), lax.axis_index("occ")
    core, x_lo = lax.rem(v, 2), lax.rem(lax.div(v, 2), 2)
    y, h = lax.div(o, 2), lax.rem(o, 2)
    y_up, y_dn, y_far = lax.rem(y + 1, n_y), lax.rem(y + n_y - 1, n_y), lax.rem(y + 2, n_y)
    z_dn = (lax.rem(v + n_vir - 4, n_vir), o)
    z_up = (lax.rem(v + 4, n_vir), o)
    x_nb = (v + 2 - 4 * x_lo, o)
    mate = (v + 1 - 2 * core, o)
    up, dn = (v, 2 * y_up + h), (v, 2 * y_dn + h)
    far = (v, o + 1 - 2 * h)

    def remote(src, dst, send, recv, to):
        return pltpu.make_async_remote_copy(
            src_ref=src, dst_ref=dst, send_sem=send, recv_sem=recv, device_id=to, device_id_type=MESH)

    def at(slot, p, s):
        return blk.at[slot, p, pl.ds(s * depth, depth)]

    def load(p, s):
        src = (tau_ref, lam_ref)[s]
        return pltpu.make_async_copy(src.at[:, pl.ds(p * LANES, LANES)], at(0, p, s), in_sem.at[2 * p + s])

    def z_copy(p, s):
        u = 2 * p + s
        return remote(at(0, p, s), at(4, p, s), zs.at[u], zr.at[u], z_dn)

    def x_copy(p, s):
        u = 2 * p + s
        return remote(at(4 - 4 * x_lo, p, s), at(2, p, s), xss.at[u], xrs.at[u], x_nb)

    def d1_copy(p, s):
        u = 2 * p + s
        return remote(at(2 - 2 * core, p, s), at(1, p, s), d1s.at[u], d1r.at[u], mate)

    def d2_copy(p, s):
        u = 2 * p + s
        return remote(at(4 - 2 * core, p, s), at(3, p, s), d2s.at[u], d2r.at[u], mate)

    def a_copy(t, j):
        src, dst, to = (
            (part.at[t, y_far, 0], r1.at[t, 0], up),
            (part.at[t, y_far, 1], r1.at[t, 1], dn),
            (part.at[t, y_up, 1], r2.at[t, 0, 1], up),
            (part.at[t, y_dn, 0], r2.at[t, 1, 0], dn),
        )[j]
        return remote(src, dst, as_.at[t, j], ar.at[t, j], to)

    def b_copy(t, j):
        return remote(s1.at[t, j], r2.at[t, j, j], bs.at[t, j], br.at[t, j], (up, dn)[j])

    def h_copy(t):
        return remote(xs.at[t], xr.at[t], hs.at[t], hr.at[t], far)

    def unit(t, i, k, p):
        acc = 0.5 * jnp.dot(lt[...], blk[k, p], preferred_element_type=F32)
        acc = acc.astype(jnp.bfloat16)
        for g in range(n_occ):
            part[t, g // 2, g % 2, i] = acc[g * rows:(g + 1) * rows]

    def send_parts(t):
        for j in range(4):
            a_copy(t, j).start()

    def pass_on(t):
        for j, near in ((0, y_up), (1, y_dn)):
            a_copy(t, j).wait_recv()
            s1[t, j] = (r1[t, j].astype(F32) + part[t, near, j].astype(F32)).astype(jnp.bfloat16)
            b_copy(t, j).start()

    def gather(t):
        for j in range(2):
            a_copy(t, 2 + j).wait_recv()
            b_copy(t, j).wait_recv()

        def total(g):
            return part[t, y, g].astype(F32) + r2[t, 0, g].astype(F32) + r2[t, 1, g].astype(F32)

        xs[t] = total(1 - h).astype(jnp.bfloat16)
        h_copy(t).start()
        fin[t] = total(h)

    for p in range(pieces):
        for s in range(2):
            load(p, s).start()

    barrier = pltpu.get_barrier_semaphore()
    for peer in (z_dn, z_up, x_nb, mate, up, dn, far):
        pl.semaphore_signal(barrier, inc=1, device_id=peer, device_id_type=MESH)
    pl.semaphore_wait(barrier, 7)

    for p in range(pieces):
        for s in range(2):
            load(p, s).wait()
            z_copy(p, s).start()

            @pl.when(x_lo == 1)
            def _():
                x_copy(p, s).start()

            @pl.when(core == 1)
            def _():
                d1_copy(p, s).start()

    for p in range(pieces):
        for s in range(2):
            lt[p * LANES:(p + 1) * LANES, (1 - s) * depth:(2 - s) * depth] = blk[0, p, s * depth:(s + 1) * depth].T

    for p in range(pieces):
        unit(0, p, 0, p)
    send_parts(0)

    def step(p, carry):
        t = p + 1
        for s in range(2):
            z_copy(p, s).wait_recv()

            @pl.when(x_lo == 0)
            def _():
                x_copy(p, s).start()

            @pl.when(core == 0)
            def _():
                d2_copy(p, s).start()

            x_copy(p, s).wait_recv()

            @pl.when(core == 0)
            def _():
                d1_copy(p, s).start()

            @pl.when(core == 1)
            def _():
                d2_copy(p, s).start()

            if s == 0:
                pass_on(t - 1)
        unit(t, 3, 4, p)
        unit(t, 1, 2, p)
        for s in range(2):
            d1_copy(p, s).wait_recv()
            d2_copy(p, s).wait_recv()
        unit(t, 0, 1, p)
        unit(t, 2, 3, p)
        send_parts(t)

        @pl.when(p > 0)
        def _():
            gather(t - 2)

        return carry

    lax.fori_loop(0, pieces, step, 0)
    pass_on(pieces)
    gather(pieces - 1)
    gather(pieces)

    for t in range(pieces + 1):
        h_copy(t).wait_recv()
        for i in range(4):
            k, p = (0, i) if t == 0 else (1 + i, t - 1)
            out_ref[k, :, p * LANES:(p + 1) * LANES] = fin[t, i] + xr[t, i].astype(F32)

    for p in range(pieces):
        for s in range(2):
            for copy in (z_copy(p, s), x_copy(p, s), d1_copy(p, s), d2_copy(p, s)):
                copy.wait_send()
    for t in range(pieces + 1):
        for j in range(4):
            a_copy(t, j).wait_send()
        for j in range(2):
            b_copy(t, j).wait_send()
        h_copy(t).wait_send()


def on_device(tau_amps, lambda_amps):
    depth, cols = tau_amps.shape
    pieces, n_occ = cols // LANES, lax.axis_size("occ")
    rows, batches, units = cols // n_occ, cols // LANES + 1, 2 * (cols // LANES)
    bf16, dma = jnp.bfloat16, pltpu.SemaphoreType.DMA
    chunk = (4, rows, LANES)
    out = pl.pallas_call(
        kernel,
        out_shape=jax.ShapeDtypeStruct((REACH + 1, rows, cols), F32),
        in_specs=[pl.BlockSpec(memory_space=pl.ANY)] * 2,
        out_specs=pl.BlockSpec(memory_space=pltpu.VMEM),
        scratch_shapes=[
            pltpu.VMEM((5, pieces, 2 * depth, LANES), bf16),
            pltpu.VMEM((cols, 2 * depth), bf16),
            pltpu.VMEM((batches, n_occ // 2, 2, *chunk), bf16),
            pltpu.VMEM((batches, 2, *chunk), bf16),
            pltpu.VMEM((batches, 2, *chunk), bf16),
            pltpu.VMEM((batches, 2, 2, *chunk), bf16),
            pltpu.VMEM((batches, *chunk), bf16),
            pltpu.VMEM((batches, *chunk), bf16),
            pltpu.VMEM((batches, *chunk), F32),
            *[dma((units,))] * 9,
            dma((batches, 4)), dma((batches, 4)),
            dma((batches, 2)), dma((batches, 2)),
            dma((batches,)), dma((batches,)),
        ],
        compiler_params=pltpu.CompilerParams(collective_id=0, has_side_effects=True),
    )(tau_amps, lambda_amps)
    return jnp.transpose(out, (1, 0, 2))


def solution(mesh):
    placed = (P("occ", "vir"), P("occ", "vir"))
    return jax.shard_map(
        on_device,
        mesh=mesh,
        in_specs=placed,
        out_specs=P(("vir", "occ"), None, None),
        check_vma=False,
    )
```

```python
import jax
import jax.numpy as jnp
from jax import lax
from jax.experimental import pallas as pl
from jax.experimental.pallas import tpu as pltpu
from jax.sharding import PartitionSpec as P

MESH = pl.DeviceIdType.MESH
REACH = 4
LANES = 128
F32 = jnp.float32


def kernel(tau_ref, lam_ref, out_ref, blk, lt, part, r1, s1, r2, xs, xr, fin,
           in_sem, zs, zr, xss, xrs, d1s, d1r, d2s, d2r, as_, ar, bs, br, hs, hr, go):
    depth = tau_ref.shape[0]
    pieces = tau_ref.shape[1] // LANES
    units = 2 * pieces
    rows = out_ref.shape[1]
    n_vir, n_occ = lax.axis_size("vir"), lax.axis_size("occ")
    n_y = n_occ // 2
    v, o = lax.axis_index("vir"), lax.axis_index("occ")
    z = lax.div(v, 4)
    core, x_lo = lax.rem(v, 2), lax.rem(lax.div(v, 2), 2)
    y, h = lax.div(o, 2), lax.rem(o, 2)
    y_up, y_dn, y_far = lax.rem(y + 1, n_y), lax.rem(y + n_y - 1, n_y), lax.rem(y + 2, n_y)
    z_dn = (lax.rem(v + n_vir - 4, n_vir), o)
    z_up = (lax.rem(v + 4, n_vir), o)
    x_nb = (v + 2 - 4 * x_lo, o)
    mate = (v + 1 - 2 * core, o)
    up, dn = (v, 2 * y_up + h), (v, 2 * y_dn + h)
    far = (v, o + 1 - 2 * h)

    def remote(src, dst, send, recv, to):
        return pltpu.make_async_remote_copy(
            src_ref=src, dst_ref=dst, send_sem=send, recv_sem=recv, device_id=to, device_id_type=MESH)

    def at(slot, p, s):
        return blk.at[slot, p, pl.ds(s * depth, depth)]

    def load(p, s):
        src = (tau_ref, lam_ref)[s]
        return pltpu.make_async_copy(src.at[:, pl.ds(p * LANES, LANES)], at(0, p, s), in_sem.at[2 * p + s])

    def z_copy(p, s):
        u = 2 * p + s
        return remote(at(0, p, s), at(4, p, s), zs.at[u], zr.at[u], z_dn)

    def x_copy(p, s):
        u = 2 * p + s
        return remote(at(4 - 4 * x_lo, p, s), at(2, p, s), xss.at[u], xrs.at[u], x_nb)

    def d1_copy(p, s):
        u = 2 * p + s
        return remote(at(2 - 2 * core, p, s), at(1, p, s), d1s.at[u], d1r.at[u], mate)

    def d2_copy(p, s):
        u = 2 * p + s
        return remote(at(4 - 2 * core, p, s), at(3, p, s), d2s.at[u], d2r.at[u], mate)

    def a_copy(t, j):
        src, dst, to = (
            (part.at[t, y_far, 0], r1.at[t, 0], up),
            (part.at[t, y_far, 1], r1.at[t, 1], dn),
            (part.at[t, y_up, 1], r2.at[t, 0, 1], up),
            (part.at[t, y_dn, 0], r2.at[t, 1, 0], dn),
        )[j]
        return remote(src, dst, as_.at[t, j], ar.at[t, j], to)

    def b_copy(t, j):
        return remote(s1.at[t, j], r2.at[t, j, j], bs.at[t, j], br.at[t, j], (up, dn)[j])

    def h_copy(t):
        return remote(xs.at[t], xr.at[t], hs.at[t], hr.at[t], far)

    def unit(t, i, k, p):
        acc = 0.5 * jnp.dot(lt[...], blk[k, p], preferred_element_type=F32)
        acc = acc.astype(jnp.bfloat16)
        for g in range(n_occ):
            part[t, g // 2, g % 2, i] = acc[g * rows:(g + 1) * rows]

    def send_parts(t):
        for j in range(4):
            a_copy(t, j).start()

    def pass_on(t):
        for j, near in ((0, y_up), (1, y_dn)):
            a_copy(t, j).wait_recv()
            s1[t, j] = (r1[t, j].astype(F32) + part[t, near, j].astype(F32)).astype(jnp.bfloat16)
            b_copy(t, j).start()

    def gather(t):
        for j in range(2):
            a_copy(t, 2 + j).wait_recv()
            b_copy(t, j).wait_recv()

        def total(g):
            return part[t, y, g].astype(F32) + r2[t, 0, g].astype(F32) + r2[t, 1, g].astype(F32)

        xs[t] = total(1 - h).astype(jnp.bfloat16)
        h_copy(t).start()
        fin[t] = total(h)

    for p in range(pieces):
        for s in range(2):
            load(p, s).start()

    barrier = pltpu.get_barrier_semaphore()
    for peer in (z_dn, x_nb, mate, up, dn, far):
        pl.semaphore_signal(barrier, inc=1, device_id=peer, device_id_type=MESH)
    pl.semaphore_wait(barrier, 6)
    pl.semaphore_signal(go, inc=1, device_id=z_up, device_id_type=MESH)

    def z_send():
        pl.semaphore_wait(go, 1)
        for p in range(pieces):
            for s in range(2):
                z_copy(p, s).start()


    for p in range(pieces):
        for s in range(2):
            load(p, s).wait()

            @pl.when(x_lo == 1)
            def _():
                x_copy(p, s).start()

            @pl.when(core == 1)
            def _():
                d1_copy(p, s).start()

    @pl.when(z > 0)
    def _():
        z_send()

    for p in range(pieces):
        for s in range(2):
            lt[p * LANES:(p + 1) * LANES, (1 - s) * depth:(2 - s) * depth] = blk[0, p, s * depth:(s + 1) * depth].T

    for t in range(2):
        for i in range(2):
            unit(t, i, 0, 2 * t + i)
        send_parts(t)
    pass_on(0)

    def step(p, carry):
        for s in range(2):
            z_copy(p, s).wait_recv()

            @pl.when(x_lo == 0)
            def _():
                x_copy(p, s).start()

            @pl.when(core == 0)
            def _():
                d2_copy(p, s).start()

            x_copy(p, s).wait_recv()

            @pl.when(core == 0)
            def _():
                d1_copy(p, s).start()

            @pl.when(core == 1)
            def _():
                d2_copy(p, s).start()

            if s == 0:
                pass_on(2 * p + 1)

        @pl.when((p == 0) & (z == 0))
        def _():
            z_send()

        unit(2 * p + 2, 0, 4, p)
        unit(2 * p + 2, 1, 2, p)
        send_parts(2 * p + 2)
        gather(2 * p)
        for s in range(2):
            d1_copy(p, s).wait_recv()
            d2_copy(p, s).wait_recv()
        unit(2 * p + 3, 0, 1, p)
        unit(2 * p + 3, 1, 3, p)
        send_parts(2 * p + 3)
        pass_on(2 * p + 2)
        gather(2 * p + 1)
        return carry

    lax.fori_loop(0, pieces, step, 0)
    pass_on(2 * pieces + 1)
    gather(2 * pieces)
    gather(2 * pieces + 1)

    for t in range(2 * pieces + 2):
        h_copy(t).wait_recv()
        for i in range(2):
            k, p = (0, 2 * t + i) if t < 2 else (((4, 2), (1, 3))[t % 2][i], t // 2 - 1)
            out_ref[k, :, p * LANES:(p + 1) * LANES] = fin[t, i] + xr[t, i].astype(F32)

    for p in range(pieces):
        for s in range(2):
            for copy in (z_copy(p, s), x_copy(p, s), d1_copy(p, s), d2_copy(p, s)):
                copy.wait_send()
    for t in range(2 * pieces + 2):
        for j in range(4):
            a_copy(t, j).wait_send()
        for j in range(2):
            b_copy(t, j).wait_send()
        h_copy(t).wait_send()


def on_device(tau_amps, lambda_amps):
    depth, cols = tau_amps.shape
    pieces, n_occ = cols // LANES, lax.axis_size("occ")
    rows, batches, units = cols // n_occ, 2 * (cols // LANES) + 2, 2 * (cols // LANES)
    bf16, dma = jnp.bfloat16, pltpu.SemaphoreType.DMA
    chunk = (2, rows, LANES)
    out = pl.pallas_call(
        kernel,
        out_shape=pltpu.VMEM((REACH + 1, rows, cols), F32),
        in_specs=[pl.BlockSpec(memory_space=pl.ANY)] * 2,
        out_specs=pl.BlockSpec(memory_space=pltpu.VMEM),
        scratch_shapes=[
            pltpu.VMEM((5, pieces, 2 * depth, LANES), bf16),
            pltpu.VMEM((cols, 2 * depth), bf16),
            pltpu.VMEM((batches, n_occ // 2, 2, *chunk), bf16),
            pltpu.VMEM((batches, 2, *chunk), bf16),
            pltpu.VMEM((batches, 2, *chunk), bf16),
            pltpu.VMEM((batches, 2, 2, *chunk), bf16),
            pltpu.VMEM((batches, *chunk), bf16),
            pltpu.VMEM((batches, *chunk), bf16),
            pltpu.VMEM((batches, *chunk), F32),
            *[dma((units,))] * 9,
            dma((batches, 4)), dma((batches, 4)),
            dma((batches, 2)), dma((batches, 2)),
            dma((batches,)), dma((batches,)),
            pltpu.SemaphoreType.REGULAR,
        ],
        compiler_params=pltpu.CompilerParams(collective_id=0, has_side_effects=True),
    )(tau_amps, lambda_amps)
    return jnp.transpose(out, (1, 0, 2))


def solution(mesh):
    placed = (P("occ", "vir"), P("occ", "vir"))
    return jax.shard_map(
        on_device,
        mesh=mesh,
        in_specs=placed,
        out_specs=P(("vir", "occ"), None, None),
        check_vma=False,
    )
```
